32 devices in a mesh: gx: 2 (over y), gy: 4 (over x, core), gz: 4 (over z).
Axes of the slice: x: 2, y: 2, z: 4, core: 2. Of those that a mesh axis runs over, the one named last changes fastest.
Arguments:
- targets: float32 [512, 512, 512], P('gx', 'gy', 'gz'), may hold values from -6 to 6
- basis_first: float32 [512, 512], replicated, may hold values from -0.25 to 0.25
- basis_second: float32 [512, 512], replicated, may hold values from -0.25 to 0.25
- basis_third: float32 [512, 512], replicated, may hold values from -0.25 to 0.25
- eigen_first: float32 [512], replicated, may hold values from 0.1 to 1
- eigen_second: float32 [512], replicated, may hold values from 0.1 to 1
- eigen_third: float32 [512], replicated, may hold values from 0.1 to 1
- noise: float32 [1], replicated, may hold values from 0.5 to 1
Outputs:
- weights: float32 [512, 512, 512], P('gx', 'gy', 'gz')
The draws below stay inside these ranges and needn't reach their ends.
All inputs are finite; a program needn't handle non-finite values.
Results may differ from the reference program's by a relative error of at most 0.000071.
Values sent between devices are 32-bit elements; how exact they have to be, the bound alone decides.
A program may use at most 128 MiB of HBM per device.

```python
import math
import jax
import jax.numpy as jnp
from jax import lax

N1 = 512
N2 = 512
N3 = 512


def steps_of(own_key, shape, shards, smallest, largest):
    def one(position, shards_of):
        heights = jax.random.uniform(jax.random.fold_in(jax.random.fold_in(own_key, 6), position), (shards_of,), jnp.float32, smallest / len(shards), largest / len(shards))
        return jnp.repeat(jnp.exp(heights), shape[position] // shards_of).reshape((-1,) + (1,) * (len(shape) - position - 1))

    loudness = one(*shards[0])
    for cut in shards[1:]:
        loudness = loudness * one(*cut)
    return loudness


def normal_values(stream_key, extent, spread, reach, split=(), kind=jnp.bfloat16):
    values = spread * jax.random.normal(stream_key, extent, jnp.float32)
    if split:
        values = values * steps_of(stream_key, extent, split, -0.22, 0.18)
    return jnp.clip(values, -reach, reach).astype(kind)


def setup_inputs(seed: int = 0) -> dict:
    streams_of = jax.random.split(jax.random.key(seed), 9)
    return {
        "targets": normal_values(streams_of[0], (N1, N2, N3), 1.0, 6.0, ((0, 2), (1, 4), (2, 4)), jnp.float32),
        "basis_first": normal_values(streams_of[1], (N1, N1), N1 ** -0.5, 0.25, (), jnp.float32),
        "basis_second": normal_values(streams_of[2], (N2, N2), N2 ** -0.5, 0.25, (), jnp.float32),
        "basis_third": normal_values(streams_of[3], (N3, N3), N3 ** -0.5, 0.25, (), jnp.float32),
        "eigen_first": jnp.clip(jnp.exp(jax.random.uniform(streams_of[4], (N1,), jnp.float32, math.log(0.1), math.log(1.0))), 0.1, 1.0),
        "eigen_second": jnp.clip(jnp.exp(jax.random.uniform(streams_of[5], (N2,), jnp.float32, math.log(0.1), math.log(1.0))), 0.1, 1.0),
        "eigen_third": jnp.clip(jnp.exp(jax.random.uniform(streams_of[6], (N3,), jnp.float32, math.log(0.1), math.log(1.0))), 0.1, 1.0),
        "noise": jnp.clip(jnp.exp(jax.random.uniform(streams_of[7], (1,), jnp.float32, math.log(0.5), math.log(1.0))), 0.5, 1.0),
    }


def reference(targets, basis_first, basis_second, basis_third, eigen_first, eigen_second, eigen_third, noise):
    high = lax.Precision.HIGHEST
    rotated = jnp.einsum('ijk,ia->ajk', targets, basis_first, precision=high)
    rotated = jnp.einsum('ajk,jb->abk', rotated, basis_second, precision=high)
    rotated = jnp.einsum('abk,kc->abc', rotated, basis_third, precision=high)
    spectrum = eigen_first[:, None, None] * eigen_second[None, :, None] * eigen_third[None, None, :] + noise[0]
    scaled = rotated / spectrum
    result = jnp.einsum('abc,kc->abk', scaled, basis_third, precision=high)
    result = jnp.einsum('abk,jb->ajk', result, basis_second, precision=high)
    result = jnp.einsum('ajk,ia->ijk', result, basis_first, precision=high)
    return result
```

```python
import jax
import jax.numpy as jnp
from jax import lax
from jax.experimental import pallas as pl
from jax.experimental.pallas import tpu as pltpu
from jax.sharding import PartitionSpec as P

MESH = pl.DeviceIdType.MESH
AHEAD = 3
SLOTS = 8
EARLY = 2
GRAIN = 8


def split(x):
    high = x.astype(jnp.bfloat16)
    low = (x - high.astype(jnp.float32)).astype(jnp.bfloat16)
    return high, low


def dot3(left, right):
    one = lambda a, b: jnp.dot(a, b, preferred_element_type=jnp.float32)
    return one(left[0], right[0]) + (one(left[0], right[1]) + one(left[1], right[0]))


def offsets_of(sizes, names):
    found = [{}]
    for name in names:
        found = [{**base, name: step} for base in found for step in range(sizes[name])]
    found = [one for one in found if any(one.values())]
    far = lambda one: min(one.get("gz", 0), sizes["gz"] - one.get("gz", 0))
    return sorted(found, key=lambda one: -far(one))


def kernel(sizes, dims, lead, b1, b2, b3, e1, e2, e3, noise, out,
           slab, made, whole, w1, w1t, w2, w2t, w3, w3t,
           base_sem, near_send, near_recv, far_send, far_recv, back_send, back_recv, out_send, out_recv):
    run, rows, cols, na, nb, n3 = dims
    me = {name: lax.axis_index(name) for name in sizes}
    shift = lambda off: {n: (lax.rem(me[n] + s, sizes[n]) if s else me[n]) for n, s in off.items()}
    near_of = lambda w: w["gx"] * sizes["gy"] + w["gy"]
    full = lambda w: {**me, **w}
    near = offsets_of(sizes, ("gx", "gy"))
    every = offsets_of(sizes, ("gz", "gx", "gy"))
    slots = min(SLOTS, run)

    i_at = lambda w: (pl.ds(pl.multiple_of(w["gx"] * rows, 8), rows), pl.ds(pl.multiple_of(w["gy"] * cols, 128), cols))
    a_from = lambda w: (w["gz"] * sizes["gx"] + w["gx"]) * na
    a_at = lambda w: (pl.ds(pl.multiple_of(a_from(w), 8), na), pl.ds(pl.multiple_of(w["gy"] * nb, 128), nb))
    k_from = lambda w: (w["gz"] * len_near + near_of(w)) * run
    len_near = sizes["gx"] * sizes["gy"]

    loads = [pltpu.make_async_copy(b, made.at[q % slots], base_sem.at[q]) for q, b in enumerate((b1, b2, b3))]
    loads[0].start()
    loads[1].start()
    barrier = pltpu.get_barrier_semaphore()
    for off in every:
        pl.semaphore_signal(barrier, inc=1, device_id=full(shift(off)), device_id_type=MESH)
    pl.semaphore_wait(barrier, len(every))

    def send_near(p):
        for off in near:
            peer = full(shift(off))
            pltpu.make_async_remote_copy(
                src_ref=lead.at[near_of(peer) * run + p], dst_ref=slab.at[(p, *i_at(me))],
                send_sem=near_send, recv_sem=near_recv.at[p], device_id=peer, device_id_type=MESH).start()
        pltpu.make_async_copy(lead.at[near_of(me) * run + p], slab.at[(p, *i_at(me))], near_recv.at[p]).start()

    def send_far(p, slot):
        for off in every:
            peer = full(shift(off))
            pltpu.make_async_remote_copy(
                src_ref=made.at[(slot, *a_at(peer))], dst_ref=whole.at[k_from(me) + p],
                send_sem=far_send.at[slot], recv_sem=far_recv, device_id=peer, device_id_type=MESH).start()

    def send_back(p, first, depth):
        piece = (pl.ds(pl.multiple_of(a_from(me) + first, 8), depth), a_at(me)[1])
        for off in every:
            peer = full(shift(off))
            pltpu.make_async_remote_copy(
                src_ref=whole.at[k_from(peer) + p, pl.ds(first, depth)], dst_ref=slab.at[(p, *piece)],
                send_sem=back_send, recv_sem=back_recv.at[p], device_id=peer, device_id_type=MESH).start()

    def send_out(p, slot):
        for off in near:
            peer = full(shift(off))
            pltpu.make_async_remote_copy(
                src_ref=made.at[(slot, *i_at(peer))], dst_ref=out.at[near_of(me) * run + p],
                send_sem=out_send.at[slot], recv_sem=out_recv, device_id=peer, device_id_type=MESH).start()
        pltpu.make_async_copy(made.at[(slot, *i_at(me))], out.at[near_of(me) * run + p], out_send.at[slot]).start()

    def await_bytes(ref, sem):
        pltpu.make_async_copy(ref, ref, sem).wait()

    def keep(pair, x):
        pair[0], pair[1] = split(x)

    for p in range(min(AHEAD, run)):
        send_near(p)

    loads[0].wait()
    loads[1].wait()
    keep(w1, made[0])
    keep(w1t, made[0].T)
    keep(w2, made[1 % slots])
    keep(w2t, made[1 % slots].T)
    loads[2].start()
    loads[2].wait()
    keep(w3, made[2 % slots])
    keep(w3t, made[2 % slots].T)

    def forward(p, carry):
        slot = lax.rem(p, slots)
        await_bytes(slab.at[p], near_recv.at[p])

        @pl.when(p >= slots)
        def _():
            await_bytes(whole.at[pl.ds(0, len(every))], far_send.at[slot])

        x = dot3(split(slab[p]), (w2[0], w2[1]))
        made[slot] = dot3((w1t[0], w1t[1]), split(x))
        send_far(p, slot)
        whole[k_from(me) + p] = made[(slot, *a_at(me))]

        @pl.when(p + AHEAD < run)
        def _():
            send_near(p + AHEAD)

        return carry

    lax.fori_loop(0, run, forward, 0)
    await_bytes(whole.at[pl.ds(0, run * len(every))], far_recv)

    second = e2[pl.ds(me["gy"], 1), :]
    third = e3[...]

    def middle(q, carry):
        first = pl.multiple_of(q * GRAIN, GRAIN)
        scale = e1[pl.ds(pl.multiple_of(a_from(me) + first, 8), GRAIN), :] * second
        scale = scale.reshape(1, GRAIN * nb)
        x = whole[:, pl.ds(first, GRAIN), :].reshape(n3, GRAIN * nb)
        x = dot3((w3t[0], w3t[1]), split(x))
        x = x / (scale * third + noise[0])
        x = dot3((w3[0], w3[1]), split(x))
        whole[:, pl.ds(first, GRAIN), :] = x.reshape(n3, GRAIN, nb)
        for p in range(min(EARLY, run)):
            send_back(p, first, GRAIN)
        return carry

    lax.fori_loop(0, na // GRAIN, middle, 0)

    def rest(p, carry):
        send_back(p, 0, na)
        return carry

    lax.fori_loop(min(EARLY, run), run, rest, 0)

    for p in range(run - slots, run):
        await_bytes(whole.at[pl.ds(0, len(every))], far_send.at[p % slots])

    def backward(p, carry):
        slot = lax.rem(p, slots)
        await_bytes(whole.at[pl.ds(0, len(every))], back_recv.at[p])
        slab[(p, *a_at(me))] = whole[k_from(me) + p]

        @pl.when(p >= slots)
        def _():
            await_bytes(lead.at[pl.ds(0, len_near)], out_send.at[slot])

        x = dot3(split(slab[p]), (w2t[0], w2t[1]))
        made[slot] = dot3((w1[0], w1[1]), split(x))
        send_out(p, slot)
        return carry

    lax.fori_loop(0, run, backward, 0)
    for p in range(run - slots, run):
        await_bytes(lead.at[pl.ds(0, len_near)], out_send.at[p % slots])
    await_bytes(lead.at[pl.ds(0, run * len(near))], near_send)
    await_bytes(whole.at[pl.ds(0, run * len(every))], back_send)
    await_bytes(lead.at[pl.ds(0, run * len(near))], out_recv)


def solution(mesh):
    sizes = {name: mesh.shape[name] for name in ("gx", "gy", "gz")}

    def per_device(targets, b1, b2, b3, e1, e2, e3, noise):
        rows, cols, deep = targets.shape
        n1, n2, n3 = b1.shape[0], b2.shape[0], b3.shape[0]
        run = deep // (sizes["gx"] * sizes["gy"])
        na, nb = n1 // (sizes["gz"] * sizes["gx"]), n2 // sizes["gy"]
        slots = min(SLOTS, run)
        lead = jnp.transpose(targets, (2, 0, 1))
        space = pl.BlockSpec(memory_space=pl.ANY)
        held = pl.BlockSpec(memory_space=pltpu.VMEM)
        dma = pltpu.SemaphoreType.DMA

        def body(*refs):
            kernel(sizes, (run, rows, cols, na, nb, n3), *refs)

        pair = lambda n: pltpu.VMEM((2, n, n), jnp.bfloat16)
        result = pl.pallas_call(
            body,
            out_shape=jax.ShapeDtypeStruct((deep, rows, cols), jnp.float32),
            in_specs=[space] * 4 + [held] * 3 + [pl.BlockSpec(memory_space=pltpu.SMEM)],
            out_specs=space,
            scratch_shapes=[
                pltpu.VMEM((run, n1, n2), jnp.float32),
                pltpu.VMEM((slots, n1, n2), jnp.float32),
                pltpu.VMEM((n3, na, nb), jnp.float32),
                pair(n1), pair(n1), pair(n2), pair(n2), pair(n3), pair(n3),
                dma((3,)), dma, dma((run,)), dma((slots,)), dma, dma, dma((run,)), dma((slots,)), dma,
            ],
            compiler_params=pltpu.CompilerParams(
                collective_id=0, has_side_effects=True, vmem_limit_bytes=67043328),
            name="solve",
        )(lead, b1, b2, b3, jnp.broadcast_to(e1[:, None], (n1, nb)), e2.reshape(-1, nb), e3[:, None], noise)
        return jnp.transpose(result, (1, 2, 0))

    return jax.shard_map(
        per_device,
        mesh=mesh,
        in_specs=(P("gx", "gy", "gz"), P(), P(), P(), P(), P(), P(), P()),
        out_specs=P("gx", "gy", "gz"),
        check_vma=False,
    )
```

```python
import jax
import jax.numpy as jnp
from jax import lax
from jax.experimental import pallas as pl
from jax.experimental.pallas import tpu as pltpu
from jax.sharding import PartitionSpec as P

MESH = pl.DeviceIdType.MESH
AHEAD = 5
SLOTS = 8
EARLY = 2
GRAIN = 8
STRIP = 16
FIRST = 1
DEPTH = 4
TURN = 32


def split(x):
    high = x.astype(jnp.bfloat16)
    low = (x - high.astype(jnp.float32)).astype(jnp.bfloat16)
    return high, low


def dot3(left, right):
    one = lambda a, b: jnp.dot(a, b, preferred_element_type=jnp.float32)
    return one(left[0], right[0]) + (one(left[0], right[1]) + one(left[1], right[0]))


def offsets_of(sizes, names):
    found = [{}]
    for name in names:
        found = [{**base, name: step} for base in found for step in range(sizes[name])]
    found = [one for one in found if any(one.values())]
    far = lambda one: min(one.get("gz", 0), sizes["gz"] - one.get("gz", 0))
    return sorted(found, key=lambda one: (-one.get("gx", 0) * sizes["gy"] - one.get("gy", 0), -far(one)))


def kernel(sizes, dims, targets, b1, b2, b3, e1, e2, e3, noise, lead, out,
           slab, made, whole, w1, w1t, w2, w2t, w3, w3t, taken, turned,
           base_sem, take_sem, turn_sem, near_send, near_recv, far_send, far_recv, back_send, back_recv, out_send, out_recv):
    run, rows, cols, na, nb, n3 = dims
    me = {name: lax.axis_index(name) for name in sizes}
    shift = lambda off: {n: (lax.rem(me[n] + s, sizes[n]) if s else me[n]) for n, s in off.items()}
    near_of = lambda w: w["gx"] * sizes["gy"] + w["gy"]
    full = lambda w: {**me, **w}
    near = offsets_of(sizes, ("gx", "gy"))
    every = offsets_of(sizes, ("gz", "gx", "gy"))
    slots = min(SLOTS, run)

    i_at = lambda w: (pl.ds(pl.multiple_of(w["gx"] * rows, 8), rows), pl.ds(pl.multiple_of(w["gy"] * cols, 128), cols))
    a_from = lambda w: (w["gz"] * sizes["gx"] + w["gx"]) * na
    a_at = lambda w: (pl.ds(pl.multiple_of(a_from(w), 8), na), pl.ds(pl.multiple_of(w["gy"] * nb, 128), nb))
    k_from = lambda w: (w["gz"] * len_near + near_of(w)) * run
    len_near = sizes["gx"] * sizes["gy"]

    deep, strip = lead.shape[0], min(STRIP, rows)
    strips, depth = rows // strip, min(DEPTH, rows // strip)
    held = [slots - 3 + q for q in range(3)]
    loads = [pltpu.make_async_copy(b, made.at[held[q]], base_sem.at[q]) for q, b in enumerate((b1, b2, b3))]
    take = lambda q: pltpu.make_async_copy(
        targets.at[pl.ds(q * strip, strip)], taken.at[lax.rem(q, depth)], take_sem.at[lax.rem(q, depth)])
    turn = lambda q: pltpu.make_async_copy(
        turned.at[lax.rem(q, depth)], lead.at[:, pl.ds(pl.multiple_of(q * strip, 8), strip)], turn_sem.at[lax.rem(q, depth)])
    for q in range(depth):
        take(q).start()
    for load in loads:
        load.start()
    barrier = pltpu.get_barrier_semaphore()
    for off in every:
        pl.semaphore_signal(barrier, inc=1, device_id=full(shift(off)), device_id_type=MESH)
    pl.semaphore_wait(barrier, len(every))

    def send_near(p, first, depth):
        piece = (pl.ds(pl.multiple_of(me["gx"] * rows + first, 8), depth), i_at(me)[1])
        part = pl.ds(pl.multiple_of(first, 8), depth)
        for off in near:
            peer = full(shift(off))
            pltpu.make_async_remote_copy(
                src_ref=lead.at[near_of(peer) * run + p, part], dst_ref=slab.at[(p, *piece)],
                send_sem=near_send, recv_sem=near_recv.at[p], device_id=peer, device_id_type=MESH).start()
        pltpu.make_async_copy(lead.at[near_of(me) * run + p, part], slab.at[(p, *piece)], near_recv.at[p]).start()

    def send_far(p, slot):
        for off in every:
            peer = full(shift(off))
            pltpu.make_async_remote_copy(
                src_ref=made.at[(slot, *a_at(peer))], dst_ref=whole.at[k_from(me) + p],
                send_sem=far_send.at[slot], recv_sem=far_recv, device_id=peer, device_id_type=MESH).start()

    def send_back(p, first, depth):
        piece = (pl.ds(pl.multiple_of(a_from(me) + first, 8), depth), a_at(me)[1])
        for off in every:
            peer = full(shift(off))
            pltpu.make_async_remote_copy(
                src_ref=whole.at[k_from(peer) + p, pl.ds(first, depth)], dst_ref=slab.at[(p, *piece)],
                send_sem=back_send, recv_sem=back_recv.at[p], device_id=peer, device_id_type=MESH).start()

    def send_out(p, slot):
        for off in near:
            peer = full(shift(off))
            pltpu.make_async_remote_copy(
                src_ref=made.at[(slot, *i_at(peer))], dst_ref=out.at[near_of(me) * run + p],
                send_sem=out_send.at[slot], recv_sem=out_recv, device_id=peer, device_id_type=MESH).start()
        pltpu.make_async_copy(made.at[(slot, *i_at(me))], out.at[near_of(me) * run + p], out_send.at[slot]).start()

    def await_bytes(ref, sem):
        pltpu.make_async_copy(ref, ref, sem).wait()

    def keep(pair, x):
        pair[0], pair[1] = split(x)

    def settle(q):
        turn(q).wait()
        for p in range(FIRST):
            send_near(p, q * strip, strip)

    def turn_strip(q, carry):
        slot = lax.rem(q, depth)
        take(q).wait()

        @pl.when(q >= depth)
        def _():
            settle(q - depth)

        turned[slot] = taken[slot].reshape(strip * cols, deep).T.reshape(deep, strip, cols)
        turn(q).start()

        @pl.when(q + depth < strips)
        def _():
            take(q + depth).start()

        return carry

    lax.fori_loop(0, strips, turn_strip, 0)
    for q in range(strips - depth, strips):
        settle(q)
    for p in range(FIRST, min(AHEAD, run)):
        send_near(p, 0, rows)
    for load in loads:
        load.wait()
    keep(w2, made[held[1]])
    keep(w1t, made[held[0]].T)

    def forward(p, carry):
        slot = lax.rem(p, slots)
        await_bytes(slab.at[p], near_recv.at[p])

        @pl.when(p >= slots)
        def _():
            await_bytes(whole.at[pl.ds(0, len(every))], far_send.at[slot])

        x = dot3(split(slab[p]), (w2[0], w2[1]))
        made[slot] = dot3((w1t[0], w1t[1]), split(x))
        send_far(p, slot)
        whole[k_from(me) + p] = made[(slot, *a_at(me))]

        @pl.when(p + AHEAD < run)
        def _():
            send_near(p + AHEAD, 0, rows)

        @pl.when(p == 0)
        def _():
            keep(w1, made[held[0]])
            keep(w2t, made[held[1]].T)
            keep(w3, made[held[2]])
            keep(w3t, made[held[2]].T)

        return carry

    lax.fori_loop(0, run, forward, 0)
    await_bytes(whole.at[pl.ds(0, run * len(every))], far_recv)

    second = e2[pl.ds(me["gy"], 1), :]
    third = jnp.broadcast_to(e3[...], (8, n3)).T[:, 0:1]

    def middle(q, carry):
        first = pl.multiple_of(q * GRAIN, GRAIN)
        scale = jnp.concatenate([e1[a_from(me) + first + s] * second for s in range(GRAIN)], axis=1)
        x = whole[:, pl.ds(first, GRAIN), :].reshape(n3, GRAIN * nb)
        x = dot3((w3t[0], w3t[1]), split(x))
        x = x / (scale * third + noise[0])
        x = dot3((w3[0], w3[1]), split(x))
        whole[:, pl.ds(first, GRAIN), :] = x.reshape(n3, GRAIN, nb)
        for p in range(min(EARLY, run)):
            send_back(p, first, GRAIN)
        return carry

    lax.fori_loop(0, na // GRAIN, middle, 0)

    def rest(p, carry):
        send_back(p, 0, na)
        return carry

    lax.fori_loop(min(EARLY, run), run, rest, 0)

    for p in range(run - slots, run):
        await_bytes(whole.at[pl.ds(0, len(every))], far_send.at[p % slots])

    def backward(p, carry):
        slot = lax.rem(p, slots)
        await_bytes(whole.at[pl.ds(0, len(every))], back_recv.at[p])
        slab[(p, *a_at(me))] = whole[k_from(me) + p]

        @pl.when(p >= slots)
        def _():
            await_bytes(lead.at[pl.ds(0, len_near)], out_send.at[slot])

        x = dot3(split(slab[p]), (w2t[0], w2t[1]))
        made[slot] = dot3((w1[0], w1[1]), split(x))
        send_out(p, slot)
        return carry

    lax.fori_loop(0, run, backward, 0)
    for p in range(run - slots, run):
        await_bytes(lead.at[pl.ds(0, len_near)], out_send.at[p % slots])
    await_bytes(lead.at[pl.ds(0, run * len(near))], near_send)
    await_bytes(whole.at[pl.ds(0, run * len(every))], back_send)
    await_bytes(lead.at[pl.ds(0, run * len(near))], out_recv)


def turn_back(x, y, taken, turned, take_sem, turn_sem):
    depth, deep, strip, cols = taken.shape
    strips = y.shape[0] // strip
    part = lambda q: pl.ds(pl.multiple_of(q * strip, 8), strip)
    take = lambda q: pltpu.make_async_copy(
        x.at[:, part(q)], taken.at[lax.rem(q, depth)], take_sem.at[lax.rem(q, depth)])
    turn = lambda q: pltpu.make_async_copy(
        turned.at[lax.rem(q, depth)], y.at[part(q)], turn_sem.at[lax.rem(q, depth)])
    for q in range(depth):
        take(q).start()

    def turn_strip(q, carry):
        slot = lax.rem(q, depth)
        take(q).wait()

        @pl.when(q >= depth)
        def _():
            turn(q - depth).wait()

        turned[slot] = taken[slot].reshape(deep, strip * cols).T.reshape(strip, cols, deep)
        turn(q).start()

        @pl.when(q + depth < strips)
        def _():
            take(q + depth).start()

        return carry

    lax.fori_loop(0, strips, turn_strip, 0)
    for q in range(strips - depth, strips):
        turn(q).wait()


def solution(mesh):
    sizes = {name: mesh.shape[name] for name in ("gx", "gy", "gz")}

    def per_device(targets, b1, b2, b3, e1, e2, e3, noise):
        rows, cols, deep = targets.shape
        n1, n2, n3 = b1.shape[0], b2.shape[0], b3.shape[0]
        run = deep // (sizes["gx"] * sizes["gy"])
        na, nb = n1 // (sizes["gz"] * sizes["gx"]), n2 // sizes["gy"]
        slots = min(SLOTS, run)
        space = pl.BlockSpec(memory_space=pl.ANY)
        held = pl.BlockSpec(memory_space=pltpu.VMEM)
        small = pl.BlockSpec(memory_space=pltpu.SMEM)
        strip, turn = min(STRIP, rows), min(TURN, rows)
        depth, back = min(DEPTH, rows // strip), min(DEPTH, rows // turn)
        spine = jax.ShapeDtypeStruct((deep, rows, cols), jnp.float32)
        dma = pltpu.SemaphoreType.DMA

        def body(*refs):
            kernel(sizes, (run, rows, cols, na, nb, n3), *refs)

        pair = lambda n: pltpu.VMEM((2, n, n), jnp.bfloat16)
        _, result = pl.pallas_call(
            body,
            out_shape=[spine, spine],
            in_specs=[space] * 4 + [small] + [held] * 2 + [small],
            out_specs=[space, space],
            scratch_shapes=[
                pltpu.VMEM((run, n1, n2), jnp.float32),
                pltpu.VMEM((slots, n1, n2), jnp.float32),
                pltpu.VMEM((n3, na, nb), jnp.float32),
                pair(n1), pair(n1), pair(n2), pair(n2), pair(n3), pair(n3),
                pltpu.VMEM((depth, strip, cols, deep), jnp.float32),
                pltpu.VMEM((depth, deep, strip, cols), jnp.float32),
                dma((3,)), dma((depth,)), dma((depth,)), dma, dma((run,)), dma((slots,)), dma, dma, dma((run,)), dma((slots,)), dma,
            ],
            compiler_params=pltpu.CompilerParams(
                collective_id=0, has_side_effects=True, vmem_limit_bytes=67043328),
            name="solve",
        )(targets, b1, b2, b3, e1, e2.reshape(-1, nb), e3.reshape(1, n3), noise)
        return pl.pallas_call(
            turn_back,
            out_shape=jax.ShapeDtypeStruct((rows, cols, deep), jnp.float32),
            in_specs=[space],
            out_specs=space,
            scratch_shapes=[
                pltpu.VMEM((back, deep, turn, cols), jnp.float32),
                pltpu.VMEM((back, turn, cols, deep), jnp.float32),
                dma((back,)), dma((back,)),
            ],
            compiler_params=pltpu.CompilerParams(vmem_limit_bytes=67043328),
            name="turn_back",
        )(result)

    return jax.shard_map(
        per_device,
        mesh=mesh,
        in_specs=(P("gx", "gy", "gz"), P(), P(), P(), P(), P(), P(), P()),
        out_specs=P("gx", "gy", "gz"),
        check_vma=False,
    )
```

```python
import jax
import jax.numpy as jnp
from jax import lax
from jax.experimental import pallas as pl
from jax.experimental.pallas import tpu as pltpu
from jax.sharding import PartitionSpec as P

MESH = pl.DeviceIdType.MESH
AHEAD = 5
SLOTS = 8
EARLY = 2
GRAIN = 8
STRIP = 16
FIRST = 1
DEPTH = 4
LAG = 2
TURN = 32


def split(x):
    high = x.astype(jnp.bfloat16)
    low = (x - high.astype(jnp.float32)).astype(jnp.bfloat16)
    return high, low


def dot3(left, right):
    one = lambda a, b: jnp.dot(a, b, preferred_element_type=jnp.float32)
    return one(left[0], right[0]) + (one(left[0], right[1]) + one(left[1], right[0]))


def offsets_of(sizes, names):
    found = [{}]
    for name in names:
        found = [{**base, name: step} for base in found for step in range(sizes[name])]
    found = [one for one in found if any(one.values())]
    core = lambda one: one.get("gy", 0) % 2
    side = lambda one: one.get("gy", 0) // 2
    hops = lambda one: (one.get("gx", 0) > 0) + (side(one) > 0)
    deep = lambda one: one.get("gz", 0)
    return sorted(found, key=lambda one: (
        -core(one), -hops(one), one.get("gx", 0), side(one),
        deep(one) < sizes["gz"] // 2, deep(one) == 0, deep(one)))


def kernel(sizes, dims, targets, b1, b2, b3, e1, e2, e3, noise, lead, out,
           slab, made, whole, w1, w1t, w2, w2t, w3, w3t, taken, turned,
           base_sem, take_sem, turn_sem, near_send, near_recv, far_send, far_recv, back_send, back_recv, out_send, out_recv):
    run, rows, cols, na, nb, n3 = dims
    me = {name: lax.axis_index(name) for name in sizes}
    paired = lambda n, s: me[n] ^ s if sizes[n] & (sizes[n] - 1) == 0 else lax.rem(me[n] + s, sizes[n])
    shift = lambda off: {n: (paired(n, s) if s else me[n]) for n, s in off.items()}
    near_of = lambda w: w["gx"] * sizes["gy"] + w["gy"]
    full = lambda w: {**me, **w}
    near = offsets_of(sizes, ("gx", "gy"))
    every = offsets_of(sizes, ("gz", "gx", "gy"))
    slots = min(SLOTS, run)

    i_at = lambda w: (pl.ds(pl.multiple_of(w["gx"] * rows, 8), rows), pl.ds(pl.multiple_of(w["gy"] * cols, 128), cols))
    a_from = lambda w: (w["gz"] * sizes["gx"] + w["gx"]) * na
    a_at = lambda w: (pl.ds(pl.multiple_of(a_from(w), 8), na), pl.ds(pl.multiple_of(w["gy"] * nb, 128), nb))
    k_from = lambda w: (w["gz"] * len_near + near_of(w)) * run
    len_near = sizes["gx"] * sizes["gy"]

    deep, strip = lead.shape[0], min(STRIP, rows)
    strips, depth = rows // strip, min(DEPTH, rows // strip)
    lag = min(LAG, depth)
    held = [slots - 3 + q for q in range(3)]
    loads = [pltpu.make_async_copy(b, made.at[held[q]], base_sem.at[q]) for q, b in enumerate((b1, b2, b3))]
    take = lambda q: pltpu.make_async_copy(
        targets.at[pl.ds(q * strip, strip)], taken.at[lax.rem(q, depth)], take_sem.at[lax.rem(q, depth)])
    turn = lambda q: pltpu.make_async_copy(
        turned.at[lax.rem(q, depth)], lead.at[:, pl.ds(pl.multiple_of(q * strip, 8), strip)], turn_sem.at[lax.rem(q, depth)])
    for q in range(depth):
        take(q).start()
    for load in loads:
        load.start()
    barrier = pltpu.get_barrier_semaphore()
    for off in every:
        pl.semaphore_signal(barrier, inc=1, device_id=full(shift(off)), device_id_type=MESH)
    pl.semaphore_wait(barrier, len(every))

    def send_near(p, first, depth):
        piece = (pl.ds(pl.multiple_of(me["gx"] * rows + first, 8), depth), i_at(me)[1])
        part = pl.ds(pl.multiple_of(first, 8), depth)
        for off in near:
            peer = full(shift(off))
            pltpu.make_async_remote_copy(
                src_ref=lead.at[near_of(peer) * run + p, part], dst_ref=slab.at[(p, *piece)],
                send_sem=near_send, recv_sem=near_recv.at[p], device_id=peer, device_id_type=MESH).start()
        pltpu.make_async_copy(lead.at[near_of(me) * run + p, part], slab.at[(p, *piece)], near_recv.at[p]).start()

    def send_far(p, slot):
        for off in every:
            peer = full(shift(off))
            pltpu.make_async_remote_copy(
                src_ref=made.at[(slot, *a_at(peer))], dst_ref=whole.at[k_from(me) + p],
                send_sem=far_send.at[slot], recv_sem=far_recv, device_id=peer, device_id_type=MESH).start()

    def send_back(p, first, depth):
        piece = (pl.ds(pl.multiple_of(a_from(me) + first, 8), depth), a_at(me)[1])
        for off in every:
            peer = full(shift(off))
            pltpu.make_async_remote_copy(
                src_ref=whole.at[k_from(peer) + p, pl.ds(first, depth)], dst_ref=slab.at[(p, *piece)],
                send_sem=back_send, recv_sem=back_recv.at[p], device_id=peer, device_id_type=MESH).start()

    def send_out(p, slot):
        for off in near:
            peer = full(shift(off))
            pltpu.make_async_remote_copy(
                src_ref=made.at[(slot, *i_at(peer))], dst_ref=out.at[near_of(me) * run + p],
                send_sem=out_send.at[slot], recv_sem=out_recv, device_id=peer, device_id_type=MESH).start()
        pltpu.make_async_copy(made.at[(slot, *i_at(me))], out.at[near_of(me) * run + p], out_send.at[slot]).start()

    def await_bytes(ref, sem):
        pltpu.make_async_copy(ref, ref, sem).wait()

    def keep(pair, x):
        pair[0], pair[1] = split(x)

    def settle(q):
        turn(q).wait()
        for p in range(FIRST):
            send_near(p, q * strip, strip)

    def turn_strip(q, carry):
        slot = lax.rem(q, depth)
        take(q).wait()

        @pl.when(q >= lag)
        def _():
            settle(q - lag)

        turned[slot] = taken[slot].reshape(strip * cols, deep).T.reshape(deep, strip, cols)
        turn(q).start()

        @pl.when(q + depth < strips)
        def _():
            take(q + depth).start()

        return carry

    lax.fori_loop(0, strips, turn_strip, 0)
    for q in range(strips - lag, strips):
        settle(q)
    for p in range(FIRST, min(AHEAD, run)):
        send_near(p, 0, rows)
    for load in loads:
        load.wait()
    keep(w2, made[held[1]])
    keep(w1t, made[held[0]].T)

    def forward(p, carry):
        slot = lax.rem(p, slots)
        await_bytes(slab.at[p], near_recv.at[p])

        @pl.when(p >= slots)
        def _():
            await_bytes(whole.at[pl.ds(0, len(every))], far_send.at[slot])

        x = dot3(split(slab[p]), (w2[0], w2[1]))
        made[slot] = dot3((w1t[0], w1t[1]), split(x))
        send_far(p, slot)
        whole[k_from(me) + p] = made[(slot, *a_at(me))]

        @pl.when(p + AHEAD < run)
        def _():
            send_near(p + AHEAD, 0, rows)

        @pl.when(p == 0)
        def _():
            keep(w1, made[held[0]])
            keep(w2t, made[held[1]].T)
            keep(w3, made[held[2]])
            keep(w3t, made[held[2]].T)

        return carry

    lax.fori_loop(0, run, forward, 0)
    await_bytes(whole.at[pl.ds(0, run * len(every))], far_recv)

    second = e2[pl.ds(me["gy"], 1), :]
    third = jnp.broadcast_to(e3[...], (8, n3)).T[:, 0:1]

    def middle(q, carry):
        first = pl.multiple_of(q * GRAIN, GRAIN)
        scale = jnp.concatenate([e1[a_from(me) + first + s] * second for s in range(GRAIN)], axis=1)
        x = whole[:, pl.ds(first, GRAIN), :].reshape(n3, GRAIN * nb)
        x = dot3((w3t[0], w3t[1]), split(x))
        x = x / (scale * third + noise[0])
        x = dot3((w3[0], w3[1]), split(x))
        whole[:, pl.ds(first, GRAIN), :] = x.reshape(n3, GRAIN, nb)
        for p in range(min(EARLY, run)):
            send_back(p, first, GRAIN)
        return carry

    lax.fori_loop(0, na // GRAIN, middle, 0)

    def rest(p, carry):
        send_back(p, 0, na)
        return carry

    lax.fori_loop(min(EARLY, run), run, rest, 0)

    for p in range(run - slots, run):
        await_bytes(whole.at[pl.ds(0, len(every))], far_send.at[p % slots])

    def backward(p, carry):
        slot = lax.rem(p, slots)
        await_bytes(whole.at[pl.ds(0, len(every))], back_recv.at[p])
        slab[(p, *a_at(me))] = whole[k_from(me) + p]

        @pl.when(p >= slots)
        def _():
            await_bytes(lead.at[pl.ds(0, len_near)], out_send.at[slot])

        x = dot3(split(slab[p]), (w2t[0], w2t[1]))
        made[slot] = dot3((w1[0], w1[1]), split(x))
        send_out(p, slot)
        return carry

    lax.fori_loop(0, run, backward, 0)
    for p in range(run - slots, run):
        await_bytes(lead.at[pl.ds(0, len_near)], out_send.at[p % slots])
    await_bytes(lead.at[pl.ds(0, run * len(near))], near_send)
    await_bytes(whole.at[pl.ds(0, run * len(every))], back_send)
    await_bytes(lead.at[pl.ds(0, run * len(near))], out_recv)


def turn_back(x, y, taken, turned, take_sem, turn_sem):
    depth, deep, strip, cols = taken.shape
    strips = y.shape[0] // strip
    part = lambda q: pl.ds(pl.multiple_of(q * strip, 8), strip)
    take = lambda q: pltpu.make_async_copy(
        x.at[:, part(q)], taken.at[lax.rem(q, depth)], take_sem.at[lax.rem(q, depth)])
    turn = lambda q: pltpu.make_async_copy(
        turned.at[lax.rem(q, depth)], y.at[part(q)], turn_sem.at[lax.rem(q, depth)])
    for q in range(depth):
        take(q).start()

    def turn_strip(q, carry):
        slot = lax.rem(q, depth)
        take(q).wait()

        @pl.when(q >= depth)
        def _():
            turn(q - depth).wait()

        turned[slot] = taken[slot].reshape(deep, strip * cols).T.reshape(strip, cols, deep)
        turn(q).start()

        @pl.when(q + depth < strips)
        def _():
            take(q + depth).start()

        return carry

    lax.fori_loop(0, strips, turn_strip, 0)
    for q in range(strips - depth, strips):
        turn(q).wait()


def solution(mesh):
    sizes = {name: mesh.shape[name] for name in ("gx", "gy", "gz")}

    def per_device(targets, b1, b2, b3, e1, e2, e3, noise):
        rows, cols, deep = targets.shape
        n1, n2, n3 = b1.shape[0], b2.shape[0], b3.shape[0]
        run = deep // (sizes["gx"] * sizes["gy"])
        na, nb = n1 // (sizes["gz"] * sizes["gx"]), n2 // sizes["gy"]
        slots = min(SLOTS, run)
        space = pl.BlockSpec(memory_space=pl.ANY)
        held = pl.BlockSpec(memory_space=pltpu.VMEM)
        small = pl.BlockSpec(memory_space=pltpu.SMEM)
        strip, turn = min(STRIP, rows), min(TURN, rows)
        depth, back = min(DEPTH, rows // strip), min(DEPTH, rows // turn)
        spine = jax.ShapeDtypeStruct((deep, rows, cols), jnp.float32)
        dma = pltpu.SemaphoreType.DMA

        def body(*refs):
            kernel(sizes, (run, rows, cols, na, nb, n3), *refs)

        pair = lambda n: pltpu.VMEM((2, n, n), jnp.bfloat16)
        _, result = pl.pallas_call(
            body,
            out_shape=[spine, spine],
            in_specs=[space] * 4 + [small] + [held] * 2 + [small],
            out_specs=[space, space],
            scratch_shapes=[
                pltpu.VMEM((run, n1, n2), jnp.float32),
                pltpu.VMEM((slots, n1, n2), jnp.float32),
                pltpu.VMEM((n3, na, nb), jnp.float32),
                pair(n1), pair(n1), pair(n2), pair(n2), pair(n3), pair(n3),
                pltpu.VMEM((depth, strip, cols, deep), jnp.float32),
                pltpu.VMEM((depth, deep, strip, cols), jnp.float32),
                dma((3,)), dma((depth,)), dma((depth,)), dma, dma((run,)), dma((slots,)), dma, dma, dma((run,)), dma((slots,)), dma,
            ],
            compiler_params=pltpu.CompilerParams(
                collective_id=0, has_side_effects=True, vmem_limit_bytes=67043328),
            name="solve",
        )(targets, b1, b2, b3, e1, e2.reshape(-1, nb), e3.reshape(1, n3), noise)
        return pl.pallas_call(
            turn_back,
            out_shape=jax.ShapeDtypeStruct((rows, cols, deep), jnp.float32),
            in_specs=[space],
            out_specs=space,
            scratch_shapes=[
                pltpu.VMEM((back, deep, turn, cols), jnp.float32),
                pltpu.VMEM((back, turn, cols, deep), jnp.float32),
                dma((back,)), dma((back,)),
            ],
            compiler_params=pltpu.CompilerParams(vmem_limit_bytes=67043328),
            name="turn_back",
        )(result)

    return jax.shard_map(
        per_device,
        mesh=mesh,
        in_specs=(P("gx", "gy", "gz"), P(), P(), P(), P(), P(), P(), P()),
        out_specs=P("gx", "gy", "gz"),
        check_vma=False,
    )
```
